32 devices in a mesh: batch: 2 (over core), neuron: 16 (over z, y, x).
Axes of the slice: x: 2, y: 2, z: 4, core: 2. Of those that a mesh axis runs over, the one named last changes fastest.
Arguments:
- images: bfloat16 [32, 65536], P('batch', 'neuron'), parts along dimension 0, may hold values from 0 to 32
- tile_weights: bfloat16 [2, 2048, 128, 128], P(None, 'neuron'), may hold values from -0.375 to 0.375
- tile_blocks: int32 [2, 2048, 2], P(None, 'neuron'), may hold values from 0 to 511, as said below
- tile_count: int32 [2, 16], P(None, 'neuron'), may hold values from 96 to 128, as said below
- bias: float32 [2, 65536], P(None, 'neuron'), may hold values from -48 to 48
Outputs:
- activity: bfloat16 [32, 65536], P('batch', 'neuron'), parts along dimension 0
The draws below stay inside these ranges and needn't reach their ends.
There are 2 independent parts, one for each index of `batch`. The reference program is written for one: setup_inputs(seed, part) draws one part's arguments, and reference() takes and returns one part's arrays. A program takes and returns all parts, laid end to end along the dimension named above; an argument that names none is the same for every part. Nothing has to cross between parts.
Inputs may be any that keep to these rules, and one draw needn't show every extreme that they name: Slots 0 to tile_count[l, d] - 1 of device d are live in layer l; in every layer one device has all 128 live. `tile_blocks`: entry [l, d * 128 + s, :] is the row block and column block of slot s of device d. Within one device and layer the column blocks are all different, and at most 8 of them lie among the 32 column blocks of any one neuron device; in every layer the column blocks of some neuron device get exactly 8 live slots from every device.
All inputs are finite; a program needn't handle non-finite values.
Results may differ from the reference program's by a relative error of at most 0.0033.
Values may be sent and summed in bfloat16 or wider, within the bound.
A program may use at most 64 MiB of HBM per device.

```python
import jax
import jax.numpy as jnp
from jax import lax

NEURONS = 65536
BLOCK = 128
LAYERS = 2
IMAGES = 16
TILES_DEV = 128
BLK_DEV = 32
SLOT_MOST = 8
N_NEURON = 16


def distinct_order(key, shape):
    scores = jax.random.randint(key, shape, 0, 65536) * shape[-1] + jnp.arange(shape[-1], dtype=jnp.int32)
    return jnp.argsort(scores, axis=-1, stable=True).astype(jnp.int32)


def draw_tile_blocks(key, part):
    base_key = jax.random.fold_in(key, 23)
    key_rows, key_owner, key_common, key_offset, key_shuffle = jax.random.split(base_key, 5)
    row_ids = jax.random.randint(key_rows, (LAYERS, N_NEURON, TILES_DEV), 0, NEURONS // BLOCK)
    owner_order = distinct_order(key_owner, (LAYERS, N_NEURON, N_NEURON))
    common = jax.random.randint(key_common, (LAYERS, 1, 1), 0, N_NEURON)
    slot_ids = jnp.arange(TILES_DEV, dtype=jnp.int32)
    groups = jnp.broadcast_to(slot_ids // SLOT_MOST, (LAYERS, N_NEURON, TILES_DEV))
    chosen = jnp.take_along_axis(owner_order, groups, axis=-1)
    owners = (chosen - owner_order[:, :, :1] + common) % N_NEURON
    offsets = jax.random.randint(key_offset, (LAYERS, N_NEURON, N_NEURON), 0, BLK_DEV)
    shifted = jnp.take_along_axis(offsets, groups, axis=-1)
    local_ids = (shifted + slot_ids % SLOT_MOST) % BLK_DEV
    col_ids = owners * BLK_DEV + local_ids
    tail_order = distinct_order(key_shuffle, (LAYERS, N_NEURON, TILES_DEV - SLOT_MOST))
    tail = jnp.take_along_axis(col_ids[:, :, SLOT_MOST:], tail_order, axis=-1)
    col_ids = jnp.concatenate([col_ids[:, :, :SLOT_MOST], tail], axis=-1)
    stacked = jnp.stack([row_ids, col_ids], axis=-1)
    return stacked.reshape(LAYERS, N_NEURON * TILES_DEV, 2).astype(jnp.int32)


def draw_tile_count(key, part):
    base_key = jax.random.fold_in(key, 11)
    key_first, key_busy = jax.random.split(base_key, 2)
    counts = jax.random.randint(key_first, (LAYERS, N_NEURON), TILES_DEV - TILES_DEV // 4, TILES_DEV + 1)
    busiest = jax.random.randint(key_busy, (LAYERS, 1), 0, N_NEURON)
    counts = jnp.where(jnp.arange(N_NEURON, dtype=jnp.int32)[None, :] == busiest, TILES_DEV, counts)
    return counts.astype(jnp.int32)


def steps_of(rng, extent, cuts, least, top_value):
    loudness, own = 1.0, jax.random.fold_in(rng, 6)
    for axis_at, parts in cuts:
        heights = jnp.exp(jax.random.uniform(jax.random.fold_in(own, axis_at), (parts,), jnp.float32, least / len(cuts), top_value / len(cuts)))
        loudness = loudness * jnp.repeat(heights, extent[axis_at] // parts).reshape([-1 if axis == axis_at else 1 for axis in range(len(extent))])
    return loudness


def gaussian(stream_key, extent, spread, reach, cuts=(), kind=jnp.bfloat16):
    values = spread * jax.random.normal(stream_key, extent, jnp.float32)
    if cuts:
        values = values * steps_of(stream_key, extent, cuts, -0.22, 0.18)
    return jnp.clip(values, -reach, reach).astype(kind)


def setup_inputs(seed: int = 0, part: int = 0) -> dict:
    key_list = jax.random.split(jax.random.key(seed), 6)
    own_keys = jax.random.split(jax.random.fold_in(key_list[5], part), 6)
    return {
        "images": jnp.clip(32.0 * jax.random.uniform(own_keys[0], (IMAGES, NEURONS), jnp.float32) ** steps_of(own_keys[0], (IMAGES, NEURONS), ((1, 16),), -0.2, 0.2), 0.0, 32.0).astype(jnp.bfloat16),
        "tile_weights": gaussian(key_list[1], (LAYERS, N_NEURON * TILES_DEV, BLOCK, BLOCK), (2 * BLOCK) ** -0.5, 0.375, ((1, 16),)),
        "tile_blocks": draw_tile_blocks(jax.random.fold_in(key_list[5], 71), part),
        "tile_count": draw_tile_count(jax.random.fold_in(key_list[5], 71), part),
        "bias": gaussian(key_list[4], (LAYERS, NEURONS), 8.0, 48.0, ((1, 16),), jnp.float32),
    }


CEILING = 32.0


def reference(images, tile_weights, tile_blocks, tile_count, bias):
    all_blocks = NEURONS // BLOCK
    activity = images
    for layer_index in range(LAYERS):
        block_view = activity.reshape(IMAGES, all_blocks, BLOCK).astype(jnp.float32)

        def device_terms(totals, pieces):
            weights, blocks, live_count = pieces
            picked = jnp.take(block_view, blocks[:, 0], axis=1)
            products = jnp.einsum("bsk,skn->sbn", picked, weights.astype(jnp.float32))
            usable = jnp.arange(TILES_DEV, dtype=jnp.int32) < live_count
            products = jnp.where(usable[:, None, None], products, jnp.zeros_like(products))
            return totals.at[blocks[:, 1]].add(products), live_count

        initial = jnp.zeros((all_blocks, IMAGES, BLOCK), jnp.float32)
        totals, unused = lax.scan(
            device_terms,
            initial,
            (
                tile_weights[layer_index].reshape(N_NEURON, TILES_DEV, BLOCK, BLOCK),
                tile_blocks[layer_index].reshape(N_NEURON, TILES_DEV, 2),
                tile_count[layer_index],
            ),
        )
        summed = jnp.transpose(totals, (1, 0, 2)).reshape(IMAGES, NEURONS)
        activity = jnp.clip(summed + bias[layer_index][None, :], 0.0, CEILING).astype(jnp.bfloat16)
    return activity
```

```python
import functools

import jax
import jax.numpy as jnp
from jax import lax
from jax.experimental import pallas as pl
from jax.experimental.pallas import tpu as pltpu
from jax.sharding import PartitionSpec as P

CEILING = 32.0
SENT = (jnp.float32, jnp.bfloat16)


def sides(devices):
    side = 1
    while 2 * side**3 < devices:
        side += 1
    if 2 * side**3 == devices:
        return 2 * side, side, side
    return devices, 1, 1


def paired(here, step, extent):
    if extent & (extent - 1):
        return lax.rem(here + step, extent)
    there, bit = 0, 1
    while bit < extent:
        there = there + (((here // bit) % 2 + (step // bit) % 2) % 2) * bit
        bit *= 2
    return there


def kernel(
    layers, devices, own, capacity,
    table, place, images, weights_hbm, bias, out,
    acts, weights, outgoing, incoming, place_in, place_smem,
    weight_sem, place_send, place_recv, smem_sem,
    z_send, z_recv, half_send, half_recv, pass_send, part_send, part_recv,
):
    me = lax.axis_index("neuron")
    zs, ys, xs = sides(devices)
    z, y, x = me // (ys * xs), (me // xs) % ys, me % xs
    slots = devices * capacity
    half = own // 2

    def index(zz, yy, xx):
        return (zz * ys + yy) * xs + xx

    def remote(src, dst, send, recv, target):
        copy = pltpu.make_async_remote_copy(
            src_ref=src, dst_ref=dst, send_sem=send, recv_sem=recv,
            device_id={"neuron": target}, device_id_type=pl.DeviceIdType.MESH,
        )
        copy.start()
        return copy

    def partner(t):
        q, i = t // (ys * xs), t % (ys * xs)
        return index(
            paired(z, zs - 1 - q, zs),
            paired(y, ys - 1 - i // xs, ys),
            paired(x, xs - 1 - i % xs, xs),
        )

    loads = []
    for layer in range(layers):
        load = pltpu.make_async_copy(weights_hbm.at[layer], weights[layer], weight_sem.at[layer])
        load.start()
        loads.append(load)

    barrier = pltpu.get_barrier_semaphore()

    def greet(t, carry):
        pl.semaphore_signal(
            barrier, inc=1, device_id={"neuron": partner(t)}, device_id_type=pl.DeviceIdType.MESH
        )
        return carry

    lax.fori_loop(0, devices - 1, greet, 0)
    for c in range(own):
        acts[0][me * own + c] = images[:, c * 128 : (c + 1) * 128]
    for layer in range(layers):
        incoming[layer][slots] = jnp.zeros(incoming[layer].shape[1:], incoming[layer].dtype)
    place_in[me] = place[me]
    pl.semaphore_wait(barrier, devices - 1)

    def place_copy(t):
        target = partner(t)
        return pltpu.make_async_remote_copy(
            src_ref=place.at[target], dst_ref=place_in.at[me],
            send_sem=place_send.at[t], recv_sem=place_recv.at[me],
            device_id={"neuron": target}, device_id_type=pl.DeviceIdType.MESH,
        )

    for layer in range(layers):
        pending = []

        def piece(owner, part):
            return acts[layer].at[pl.ds(owner * own + part * half, half)]

        def arrived(ref, sem):
            pltpu.make_async_copy(ref, ref, sem).wait()

        mine = acts[layer].at[pl.ds(me * own, own)]
        for m in range(1, zs):
            pending.append(
                remote(mine, mine, z_send.at[layer, m], z_recv.at[layer, z],
                       index(paired(z, m, zs), y, x))
            )

        def spread(m):
            zz = paired(z, m, zs)
            owner = index(zz, y, x)
            if m:
                shard = acts[layer].at[pl.ds(owner * own, own)]
                arrived(shard, z_recv.at[layer, zz])
            slot = 0
            for first in (True, False):
                for n in range(1, ys):
                    part = 0 if first else 1
                    pending.append(
                        remote(piece(owner, part), piece(owner, part),
                               half_send.at[layer, m, slot], half_recv.at[layer, owner, part],
                               index(z, paired(y, n, ys), x))
                    )
                    slot += 1
                for n in range(1, xs):
                    part = 1 if first else 0
                    pending.append(
                        remote(piece(owner, part), piece(owner, part),
                               half_send.at[layer, m, slot], half_recv.at[layer, owner, part],
                               index(z, y, paired(x, n, xs)))
                    )
                    slot += 1

        def relay(m):
            zz = paired(z, m, zs)
            slot = 0
            for n in range(1, ys):
                owner = index(zz, paired(y, n, ys), x)
                arrived(piece(owner, 0), half_recv.at[layer, owner, 0])
                for k in range(1, xs):
                    pending.append(
                        remote(piece(owner, 0), piece(owner, 0),
                               pass_send.at[layer, m, slot], half_recv.at[layer, owner, 0],
                               index(z, y, paired(x, k, xs)))
                    )
                    slot += 1
            for n in range(1, xs):
                owner = index(zz, y, paired(x, n, xs))
                arrived(piece(owner, 1), half_recv.at[layer, owner, 1])
                for k in range(1, ys):
                    pending.append(
                        remote(piece(owner, 1), piece(owner, 1),
                               pass_send.at[layer, m, slot], half_recv.at[layer, owner, 1],
                               index(z, paired(y, k, ys), x))
                    )
                    slot += 1

        spread(0)
        if layer == 0:
            def send_place(t, carry):
                place_copy(t).start()
                return carry

            lax.fori_loop(0, devices - 1, send_place, 0)
        for m in range(1, zs):
            spread(m)
            relay(m - 1)
        relay(zs - 1)

        for m in range(zs):
            zz = paired(z, m, zs)
            for n in range(1, ys):
                owner = index(zz, paired(y, n, ys), x)
                arrived(piece(owner, 1), half_recv.at[layer, owner, 1])
            for n in range(1, xs):
                owner = index(zz, y, paired(x, n, xs))
                arrived(piece(owner, 0), half_recv.at[layer, owner, 0])
            for n in range(1, ys):
                for k in range(1, xs):
                    owner = index(zz, paired(y, n, ys), paired(x, k, xs))
                    for part in range(2):
                        arrived(piece(owner, part), half_recv.at[layer, owner, part])
        loads[layer].wait()

        out_buf, in_buf = outgoing[layer], incoming[layer]

        def product(target, k):
            at = layer * 2 * slots + target * capacity + k
            block = acts[layer][table[at]]
            tile = weights[layer][table[at + slots]]
            return jnp.dot(block, tile, preferred_element_type=jnp.float32).astype(out_buf.dtype)

        def part_copy(t):
            target = partner(t)
            return pltpu.make_async_remote_copy(
                src_ref=out_buf.at[pl.ds(target * capacity, capacity)],
                dst_ref=in_buf.at[pl.ds(me * capacity, capacity)],
                send_sem=part_send.at[layer, t], recv_sem=part_recv.at[layer, me],
                device_id={"neuron": target}, device_id_type=pl.DeviceIdType.MESH,
            )

        def step(t, carry):
            target = partner(t)
            for k in range(capacity):
                out_buf[target * capacity + k] = product(target, k)
            part_copy(t).start()
            return carry

        lax.fori_loop(0, devices - 1, step, 0)
        for k in range(capacity):
            in_buf[me * capacity + k] = product(me, k)

        if layer == 0:
            def take_place(t, carry):
                ref = place_in.at[partner(t)]
                pltpu.make_async_copy(ref, ref, place_recv.at[partner(t)]).wait()
                return carry

            lax.fori_loop(0, devices - 1, take_place, 0)
            to_smem = pltpu.make_async_copy(place_in, place_smem, smem_sem)
            to_smem.start()
            to_smem.wait()

        def take_part(t, carry):
            source = partner(t)
            ref = in_buf.at[pl.ds(source * capacity, capacity)]
            pltpu.make_async_copy(ref, ref, part_recv.at[layer, source]).wait()
            return carry

        lax.fori_loop(0, devices - 1, take_part, 0)

        def combine(c, carry):
            total = jnp.broadcast_to(
                bias[pl.ds(layer, 1), pl.ds(pl.multiple_of(c * 128, 128), 128)], in_buf.shape[1:]
            )
            for source in range(devices):
                at = place_smem[source, 0, layer * own + c]
                total = total + in_buf[at].astype(jnp.float32)
            value = jnp.minimum(jnp.maximum(total, 0.0), CEILING).astype(jnp.bfloat16)
            if layer + 1 < layers:
                acts[layer + 1][me * own + c] = value
            else:
                out[:, pl.ds(pl.multiple_of(c * 128, 128), 128)] = value
            return carry

        lax.fori_loop(0, own, combine, 0)

        for copy in pending:
            copy.wait_send()

        def drain(t, carry):
            part_copy(t).wait_send()
            if layer == 0:
                place_copy(t).wait_send()
            return carry

        lax.fori_loop(0, devices - 1, drain, 0)


def tables(tile_blocks, tile_count, devices, own, capacity):
    layers, slot_total, _ = tile_blocks.shape
    me = lax.axis_index("neuron")
    slots = devices * capacity
    row_ids, col_ids = tile_blocks[:, :, 0], tile_blocks[:, :, 1]
    slot_ids = jnp.arange(slot_total, dtype=jnp.int32)
    usable = slot_ids[None, :] < tile_count
    owners = jnp.where(usable, col_ids // own, -1)
    earlier = (owners[:, :, None] == owners[:, None, :]) & (slot_ids[None, :] < slot_ids[:, None])
    rank = jnp.sum(earlier.astype(jnp.int32), axis=2)
    dest = jnp.where(usable, owners * capacity + rank, -1)
    hit = dest[:, None, :] == jnp.arange(slots, dtype=jnp.int32)[:, None]
    rows = jnp.sum(jnp.where(hit, row_ids[:, None, :], 0), axis=2)
    tiles = jnp.sum(jnp.where(hit, slot_ids, 0), axis=2)
    table = jnp.stack([rows, tiles], axis=1).reshape(-1)
    live_cols = jnp.where(usable, col_ids, -1)
    match = live_cols[:, None, :] == jnp.arange(devices * own, dtype=jnp.int32)[:, None]
    place = slots + jnp.sum(jnp.where(match, me * capacity + rank[:, None, :] - slots, 0), axis=2)
    place = jnp.transpose(place.reshape(layers, devices, own), (1, 0, 2)).reshape(devices, 1, layers * own)
    width = -(-layers * own // 128) * 128
    return table, jnp.pad(place, ((0, 0), (0, 0), (0, width - layers * own)))


def local(images, tile_weights, tile_blocks, tile_count, bias):
    devices = lax.axis_size("neuron")
    layers, slot_total, block, _ = tile_weights.shape
    image_rows, local_width = images.shape
    own = local_width // block
    capacity = max(2, slot_total // devices)
    slots = devices * capacity
    zs, ys, xs = sides(devices)
    table, place = tables(tile_blocks, tile_count, devices, own, capacity)
    width = place.shape[2]
    sent = [SENT[min(layer, len(SENT) - 1)] for layer in range(layers)]
    fan = 2 * (ys + xs)
    vmem = pl.BlockSpec(memory_space=pltpu.VMEM)
    return pl.pallas_call(
        functools.partial(kernel, layers, devices, own, capacity),
        out_shape=jax.ShapeDtypeStruct((image_rows, local_width), jnp.bfloat16),
        in_specs=[
            pl.BlockSpec(memory_space=pltpu.SMEM), vmem, vmem,
            pl.BlockSpec(memory_space=pl.ANY), vmem,
        ],
        out_specs=vmem,
        scratch_shapes=[
            [pltpu.VMEM((devices * own, image_rows, block), jnp.bfloat16)] * layers,
            [pltpu.VMEM((slot_total, block, block), jnp.bfloat16)] * layers,
            [pltpu.VMEM((slots, image_rows, block), kind) for kind in sent],
            [pltpu.VMEM((slots + 1, image_rows, block), kind) for kind in sent],
            pltpu.VMEM((devices, 1, width), jnp.int32),
            pltpu.SMEM((devices, 1, width), jnp.int32),
            pltpu.SemaphoreType.DMA((layers,)),
            pltpu.SemaphoreType.DMA((devices,)),
            pltpu.SemaphoreType.DMA((devices,)),
            pltpu.SemaphoreType.DMA,
            pltpu.SemaphoreType.DMA((layers, zs)),
            pltpu.SemaphoreType.DMA((layers, zs)),
            pltpu.SemaphoreType.DMA((layers, zs, fan)),
            pltpu.SemaphoreType.DMA((layers, devices, 2)),
            pltpu.SemaphoreType.DMA((layers, zs, 2 * ys * xs)),
            pltpu.SemaphoreType.DMA((layers, devices)),
            pltpu.SemaphoreType.DMA((layers, devices)),
        ],
        compiler_params=pltpu.CompilerParams(
            collective_id=0, has_side_effects=True, vmem_limit_bytes=48 * 1024 * 1024
        ),
    )(table, place, images, tile_weights, bias)


def solution(mesh):
    in_specs = (
        P("batch", "neuron"),
        P(None, "neuron", None, None),
        P(None, "neuron", None),
        P(None, "neuron"),
        P(None, "neuron"),
    )
    out_specs = P("batch", "neuron")
    return jax.shard_map(local, mesh=mesh, in_specs=in_specs, out_specs=out_specs, check_vma=False)
```

```python
import functools

import jax
import jax.numpy as jnp
from jax import lax
from jax.experimental import pallas as pl
from jax.experimental.pallas import tpu as pltpu
from jax.sharding import PartitionSpec as P

CEILING = 32.0
NEAR, FAR = jnp.float32, jnp.bfloat16
GROUP = 4


def sides(devices):
    side = 1
    while 2 * side**3 < devices:
        side += 1
    if 2 * side**3 == devices:
        return 2 * side, side, side
    return devices, 1, 1


def paired(here, step, extent):
    if extent & (extent - 1):
        return lax.rem(here + step, extent)
    there, bit = 0, 1
    while bit < extent:
        there = there + (((here // bit) % 2 + (step // bit) % 2) % 2) * bit
        bit *= 2
    return there


def kernel(
    layers, devices, own, capacity,
    counts, blocks, images, weights_hbm, bias, out,
    acts, weights, far_out, near_out, far_in, near_in, table_out, table, place, place_in, place_smem,
    weight_sem, place_send, place_recv, smem_sem,
    z_send, z_recv, half_send, half_recv, pass_send, part_send, part_recv,
):
    me = lax.axis_index("neuron")
    zs, ys, xs = sides(devices)
    z, y, x = me // (ys * xs), (me // xs) % ys, me % xs
    slots = devices * capacity
    half = own // 2

    def index(zz, yy, xx):
        return (zz * ys + yy) * xs + xx

    def remote(src, dst, send, recv, target):
        copy = pltpu.make_async_remote_copy(
            src_ref=src, dst_ref=dst, send_sem=send, recv_sem=recv,
            device_id={"neuron": target}, device_id_type=pl.DeviceIdType.MESH,
        )
        copy.start()
        return copy

    far = devices // 2

    def partner(t):
        return paired(me, devices - 1 - t, devices)

    loads = []
    for layer in range(layers):
        load = pltpu.make_async_copy(weights_hbm.at[layer], weights[layer], weight_sem.at[layer])
        load.start()
        loads.append(load)

    barrier = pltpu.get_barrier_semaphore()

    def greet(t, carry):
        pl.semaphore_signal(
            barrier, inc=1, device_id={"neuron": partner(t)}, device_id_type=pl.DeviceIdType.MESH
        )
        return carry

    lax.fori_loop(0, devices - 1, greet, 0)
    for c in range(own):
        acts[0][me * own + c] = images[:, c * 128 : (c + 1) * 128]
    for layer in range(layers):
        for buf in (far_in[layer], near_in[layer]):
            buf[far * capacity] = jnp.zeros(buf.shape[1:], buf.dtype)
    pl.semaphore_wait(barrier, devices - 1)
    chunk_at = lax.rem(me * own, 128)

    def place_copy(t):
        target = partner(t)
        return pltpu.make_async_remote_copy(
            src_ref=place.at[(target * own) // 128], dst_ref=place_in.at[me],
            send_sem=place_send.at[t], recv_sem=place_recv.at[me],
            device_id={"neuron": target}, device_id_type=pl.DeviceIdType.MESH,
        )

    def make_tables():
        total = blocks.shape[1]
        for layer in range(layers):
            both = blocks[layer]
            row_of, col_of = both[:, 0:1], both[:, 1:2]
            slot_of = lax.broadcasted_iota(jnp.int32, (total, total), 0)
            other = lax.broadcasted_iota(jnp.int32, (total, total), 1)
            usable = slot_of[:, 0:1] < counts[layer, 0]
            owner = jnp.where(usable, col_of // own, -1)
            wide = jnp.broadcast_to(owner, (total, total)).astype(jnp.float32)
            same = (wide == wide.T) & (other < slot_of)
            rank = jnp.sum(jnp.where(same, 1.0, 0.0), axis=1, keepdims=True).astype(jnp.int32)
            spot = jnp.where(usable, owner * capacity + rank, -1)
            hit = spot == lax.broadcasted_iota(jnp.int32, (total, slots), 1)
            table_out[2 * layer] = jnp.sum(jnp.where(hit, row_of, 0), axis=0, keepdims=True)
            table_out[2 * layer + 1] = jnp.sum(
                jnp.where(hit, slot_of[:, 0:1], 0), axis=0, keepdims=True
            )
            empty = far * capacity
            column = jnp.where(usable, col_of, -1)
            term = paired_term(owner) * capacity + rank - empty
            for chunk in range(devices * own // 128):
                lane = lax.broadcasted_iota(jnp.int32, (total, 128), 1) + chunk * 128
                place[chunk, layer] = empty + jnp.sum(
                    jnp.where(column == lane, term, 0), axis=0, keepdims=True
                )

    def paired_term(owner):
        distance, bit = jnp.zeros_like(owner), 1
        while bit < devices:
            distance = distance + jnp.where((owner // bit) % 2 == (me // bit) % 2, 0, bit)
            bit *= 2
        return lax.rem(devices - 1 - distance, far)

    for layer in range(layers):
        pending = []

        def piece(owner, part):
            return acts[layer].at[pl.ds(owner * own + part * half, half)]

        def arrived(ref, sem):
            pltpu.make_async_copy(ref, ref, sem).wait()

        mine = acts[layer].at[pl.ds(me * own, own)]
        for m in range(1, zs):
            pending.append(
                remote(mine, mine, z_send.at[layer, m], z_recv.at[layer, z],
                       index(paired(z, m, zs), y, x))
            )

        def spread(m):
            zz = paired(z, m, zs)
            owner = index(zz, y, x)
            if m:
                shard = acts[layer].at[pl.ds(owner * own, own)]
                arrived(shard, z_recv.at[layer, zz])
            slot = 0
            for first in (True, False):
                for n in range(1, ys):
                    part = 0 if first else 1
                    pending.append(
                        remote(piece(owner, part), piece(owner, part),
                               half_send.at[layer, m, slot], half_recv.at[layer, owner, part],
                               index(z, paired(y, n, ys), x))
                    )
                    slot += 1
                for n in range(1, xs):
                    part = 1 if first else 0
                    pending.append(
                        remote(piece(owner, part), piece(owner, part),
                               half_send.at[layer, m, slot], half_recv.at[layer, owner, part],
                               index(z, y, paired(x, n, xs)))
                    )
                    slot += 1

        def relay(m):
            zz = paired(z, m, zs)
            slot = 0
            for n in range(1, ys):
                owner = index(zz, paired(y, n, ys), x)
                arrived(piece(owner, 0), half_recv.at[layer, owner, 0])
                for k in range(1, xs):
                    pending.append(
                        remote(piece(owner, 0), piece(owner, 0),
                               pass_send.at[layer, m, slot], half_recv.at[layer, owner, 0],
                               index(z, y, paired(x, k, xs)))
                    )
                    slot += 1
            for n in range(1, xs):
                owner = index(zz, y, paired(x, n, xs))
                arrived(piece(owner, 1), half_recv.at[layer, owner, 1])
                for k in range(1, ys):
                    pending.append(
                        remote(piece(owner, 1), piece(owner, 1),
                               pass_send.at[layer, m, slot], half_recv.at[layer, owner, 1],
                               index(z, paired(y, k, ys), x))
                    )
                    slot += 1

        spread(0)
        if layer == 0:
            make_tables()
            place_in[me] = place[(me * own) // 128]
            to_table = pltpu.make_async_copy(table_out, table, smem_sem)
            to_table.start()
            to_table.wait()

            def send_place(t, carry):
                place_copy(t).start()
                return carry

            lax.fori_loop(0, devices - 1, send_place, 0)
        for m in range(1, zs):
            spread(m)
            relay(m - 1)
        relay(zs - 1)

        for m in range(zs):
            zz = paired(z, m, zs)
            for n in range(1, ys):
                owner = index(zz, paired(y, n, ys), x)
                arrived(piece(owner, 1), half_recv.at[layer, owner, 1])
            for n in range(1, xs):
                owner = index(zz, y, paired(x, n, xs))
                arrived(piece(owner, 0), half_recv.at[layer, owner, 0])
            for n in range(1, ys):
                for k in range(1, xs):
                    owner = index(zz, paired(y, n, ys), paired(x, k, xs))
                    for part in range(2):
                        arrived(piece(owner, part), half_recv.at[layer, owner, part])
        loads[layer].wait()

        def product(target, k, kind):
            at = target * capacity + k
            block = acts[layer][table[2 * layer, 0, at]]
            tile = weights[layer][table[2 * layer + 1, 0, at]]
            return jnp.dot(block, tile, preferred_element_type=jnp.float32).astype(kind)

        def buffers(is_far):
            if is_far:
                return far_out[layer], far_in[layer], 0
            return near_out[layer], near_in[layer], far

        def part_copy(t, is_far):
            sent, got, base = buffers(is_far)
            rows = pl.ds((t - base) * capacity, capacity)
            return pltpu.make_async_remote_copy(
                src_ref=sent.at[rows], dst_ref=got.at[rows],
                send_sem=part_send.at[layer, t], recv_sem=part_recv.at[layer, t],
                device_id={"neuron": partner(t)}, device_id_type=pl.DeviceIdType.MESH,
            )

        def fill(t, is_far, to):
            target = partner(t)
            base = buffers(is_far)[2]
            for k in range(capacity):
                to[(t - base) * capacity + k] = product(target, k, to.dtype)

        group = GROUP if far % GROUP == 0 else 1

        def step(is_far, base, g, carry):
            for i in range(group):
                fill(base + g * group + i, is_far, buffers(is_far)[0])
            for i in range(group):
                part_copy(base + g * group + i, is_far).start()
            return carry

        lax.fori_loop(0, far // group, functools.partial(step, True, 0), 0)
        lax.fori_loop(0, far // group - 1, functools.partial(step, False, far), 0)
        for t in range(devices - group, devices - 1):
            fill(t, False, near_out[layer])
        for t in range(devices - group, devices - 1):
            part_copy(t, False).start()
        fill(devices - 1, False, near_in[layer])

        if layer == 0:
            def take_place(t, carry):
                ref = place_in.at[partner(t)]
                pltpu.make_async_copy(ref, ref, place_recv.at[partner(t)]).wait()
                return carry

            lax.fori_loop(0, devices - 1, take_place, 0)
            to_smem = pltpu.make_async_copy(place_in, place_smem, smem_sem)
            to_smem.start()
            to_smem.wait()

        def take_part(is_far, t, carry):
            part_copy(t, is_far).wait_recv()
            return carry

        lax.fori_loop(far, devices - 1, functools.partial(take_part, False), 0)
        lax.fori_loop(0, far, functools.partial(take_part, True), 0)

        def combine(c, carry):
            total = jnp.broadcast_to(
                bias[pl.ds(layer, 1), pl.ds(pl.multiple_of(c * 128, 128), 128)],
                near_in[layer].shape[1:],
            )
            for t in range(devices):
                at = place_smem[partner(t), layer, 0, chunk_at + c]
                total = total + buffers(t < far)[1][at].astype(jnp.float32)
            value = jnp.minimum(jnp.maximum(total, 0.0), CEILING).astype(jnp.bfloat16)
            if layer + 1 < layers:
                acts[layer + 1][me * own + c] = value
            else:
                out[:, pl.ds(pl.multiple_of(c * 128, 128), 128)] = value
            return carry

        lax.fori_loop(0, own, combine, 0)

        for copy in pending:
            copy.wait_send()

        def drain(is_far, t, carry):
            part_copy(t, is_far).wait_send()
            if layer == 0:
                place_copy(t).wait_send()
            return carry

        lax.fori_loop(0, far, functools.partial(drain, True), 0)
        lax.fori_loop(far, devices - 1, functools.partial(drain, False), 0)


def local(images, tile_weights, tile_blocks, tile_count, bias):
    devices = lax.axis_size("neuron")
    layers, slot_total, block, _ = tile_weights.shape
    image_rows, local_width = images.shape
    own = local_width // block
    capacity = max(2, slot_total // devices)
    slots = devices * capacity
    zs, ys, xs = sides(devices)
    half_slots = slots // 2
    chunks = devices * own // 128
    fan = 2 * (ys + xs)
    vmem = pl.BlockSpec(memory_space=pltpu.VMEM)
    return pl.pallas_call(
        functools.partial(kernel, layers, devices, own, capacity),
        out_shape=jax.ShapeDtypeStruct((image_rows, local_width), jnp.bfloat16),
        in_specs=[
            pl.BlockSpec(memory_space=pltpu.SMEM), vmem, vmem,
            pl.BlockSpec(memory_space=pl.ANY), vmem,
        ],
        out_specs=vmem,
        scratch_shapes=[
            [pltpu.VMEM((devices * own, image_rows, block), jnp.bfloat16)] * layers,
            [pltpu.VMEM((slot_total, block, block), jnp.bfloat16)] * layers,
            [pltpu.VMEM((half_slots, image_rows, block), FAR)] * layers,
            [pltpu.VMEM((half_slots, image_rows, block), NEAR)] * layers,
            [pltpu.VMEM((half_slots + 1, image_rows, block), FAR)] * layers,
            [pltpu.VMEM((half_slots + 1, image_rows, block), NEAR)] * layers,
            pltpu.VMEM((2 * layers, 1, slots), jnp.int32),
            pltpu.SMEM((2 * layers, 1, slots), jnp.int32),
            pltpu.VMEM((chunks, layers, 1, 128), jnp.int32),
            pltpu.VMEM((devices, layers, 1, 128), jnp.int32),
            pltpu.SMEM((devices, layers, 1, 128), jnp.int32),
            pltpu.SemaphoreType.DMA((layers,)),
            pltpu.SemaphoreType.DMA((devices,)),
            pltpu.SemaphoreType.DMA((devices,)),
            pltpu.SemaphoreType.DMA,
            pltpu.SemaphoreType.DMA((layers, zs)),
            pltpu.SemaphoreType.DMA((layers, zs)),
            pltpu.SemaphoreType.DMA((layers, zs, fan)),
            pltpu.SemaphoreType.DMA((layers, devices, 2)),
            pltpu.SemaphoreType.DMA((layers, zs, 2 * ys * xs)),
            pltpu.SemaphoreType.DMA((layers, devices)),
            pltpu.SemaphoreType.DMA((layers, devices)),
        ],
        compiler_params=pltpu.CompilerParams(
            collective_id=0, has_side_effects=True, vmem_limit_bytes=48 * 1024 * 1024
        ),
    )(tile_count, tile_blocks, images, tile_weights, bias)


def solution(mesh):
    in_specs = (
        P("batch", "neuron"),
        P(None, "neuron", None, None),
        P(None, "neuron", None),
        P(None, "neuron"),
        P(None, "neuron"),
    )
    out_specs = P("batch", "neuron")
    return jax.shard_map(local, mesh=mesh, in_specs=in_specs, out_specs=out_specs, check_vma=False)
```

```python
import functools

import jax
import jax.numpy as jnp
from jax import lax
from jax.experimental import pallas as pl
from jax.experimental.pallas import tpu as pltpu
from jax.sharding import PartitionSpec as P

CEILING = 32.0
NEAR, FAR = jnp.float32, jnp.bfloat16
GROUP = 4


def sides(devices):
    side = 1
    while 2 * side**3 < devices:
        side += 1
    if 2 * side**3 == devices:
        return 2 * side, side, side
    return devices, 1, 1


def paired(here, step, extent):
    if extent & (extent - 1):
        return lax.rem(here + step, extent)
    there, bit = 0, 1
    while bit < extent:
        there = there + (((here // bit) % 2 + (step // bit) % 2) % 2) * bit
        bit *= 2
    return there


def kernel(
    layers, devices, own, capacity,
    counts, blocks, images_hbm, weights_hbm, bias_hbm, out,
    acts, weights, far_out, near_out, far_in, near_in, table_out, table, place, place_in, place_smem,
    images, bias, sums, early_sem, weight_sem, place_send, place_recv, smem_sem,
    z_send, z_recv, half_send, half_recv, pass_send, part_send, part_recv, side_send, side_pass, side_recv,
):
    me = lax.axis_index("neuron")
    zs, ys, xs = sides(devices)
    z, y, x = me // (ys * xs), (me // xs) % ys, me % xs
    slots = devices * capacity
    side = own // 8
    main = own - side
    half = main // 2

    def index(zz, yy, xx):
        return (zz * ys + yy) * xs + xx

    def remote(src, dst, send, recv, target):
        copy = pltpu.make_async_remote_copy(
            src_ref=src, dst_ref=dst, send_sem=send, recv_sem=recv,
            device_id={"neuron": target}, device_id_type=pl.DeviceIdType.MESH,
        )
        copy.start()
        return copy

    far = devices // 2

    def partner(t):
        return paired(me, devices - 1 - t, devices)

    early = [
        pltpu.make_async_copy(images_hbm, images, early_sem.at[0]),
        pltpu.make_async_copy(bias_hbm, bias, early_sem.at[1]),
    ]
    for load in early:
        load.start()
    loads = []
    for layer in range(layers):
        load = pltpu.make_async_copy(weights_hbm.at[layer], weights[layer], weight_sem.at[layer])
        load.start()
        loads.append(load)

    barrier = pltpu.get_barrier_semaphore()

    def greet(t, carry):
        pl.semaphore_signal(
            barrier, inc=1, device_id={"neuron": partner(t)}, device_id_type=pl.DeviceIdType.MESH
        )
        return carry

    lax.fori_loop(0, devices - 1, greet, 0)
    early[0].wait()
    for c in range(own):
        acts[0][me * own + c] = images[:, c * 128 : (c + 1) * 128]
    for layer in range(layers):
        for buf in (far_in[layer], near_in[layer]):
            buf[far * capacity] = jnp.zeros(buf.shape[1:], buf.dtype)
    pl.semaphore_wait(barrier, devices - 1)
    chunk_at = lax.rem(me * own, 128)

    def place_copy(t):
        target = partner(t)
        return pltpu.make_async_remote_copy(
            src_ref=place.at[(target * own) // 128], dst_ref=place_in.at[me],
            send_sem=place_send.at[t], recv_sem=place_recv.at[me],
            device_id={"neuron": target}, device_id_type=pl.DeviceIdType.MESH,
        )

    def make_tables():
        total = blocks.shape[2]
        for layer in range(layers):
            row_of, col_of = (
                jnp.broadcast_to(blocks[layer, i : i + 1, :], (total, total))
                .astype(jnp.float32).T.astype(jnp.int32)[:, 0:1]
                for i in range(2)
            )
            slot_of = lax.broadcasted_iota(jnp.int32, (total, total), 0)
            other = lax.broadcasted_iota(jnp.int32, (total, total), 1)
            usable = slot_of[:, 0:1] < counts[layer]
            owner = jnp.where(usable, col_of // own, -1)
            wide = jnp.broadcast_to(owner, (total, total)).astype(jnp.float32)
            same = (wide == wide.T) & (other < slot_of)
            rank = jnp.sum(jnp.where(same, 1.0, 0.0), axis=1, keepdims=True).astype(jnp.int32)
            spot = jnp.where(usable, owner * capacity + rank, -1)
            hit = spot == lax.broadcasted_iota(jnp.int32, (total, slots), 1)
            table_out[2 * layer] = jnp.sum(jnp.where(hit, row_of, 0), axis=0, keepdims=True)
            table_out[2 * layer + 1] = jnp.sum(
                jnp.where(hit, slot_of[:, 0:1], 0), axis=0, keepdims=True
            )
            empty = far * capacity
            column = jnp.where(usable, col_of, -1)
            term = paired_term(owner) * capacity + rank - empty
            for chunk in range(devices * own // 128):
                lane = lax.broadcasted_iota(jnp.int32, (total, 128), 1) + chunk * 128
                place[chunk, layer] = empty + jnp.sum(
                    jnp.where(column == lane, term, 0), axis=0, keepdims=True
                )

    def paired_term(owner):
        distance, bit = jnp.zeros_like(owner), 1
        while bit < devices:
            distance = distance + jnp.where((owner // bit) % 2 == (me // bit) % 2, 0, bit)
            bit *= 2
        return lax.rem(devices - 1 - distance, far)

    for layer in range(layers):
        pending = []

        def piece(owner, part):
            return acts[layer].at[pl.ds(owner * own + part * half, half)]

        def arrived(ref, sem):
            pltpu.make_async_copy(ref, ref, sem).wait()

        def side_of(owner):
            return acts[layer].at[pl.ds(owner * own + main, side)]

        def side_along_z(owner, row):
            for m in range(1, zs):
                pending.append(
                    remote(side_of(owner), side_of(owner), side_pass.at[layer, row, m],
                           side_recv.at[layer, owner], index(paired(z, m, zs), y, x))
                )

        mates = [(n, k) for n in range(ys) for k in range(xs) if n or k]

        def mate(zz, row):
            return index(zz, paired(y, mates[row][0], ys), paired(x, mates[row][1], xs))

        if side:
            for row in range(len(mates)):
                pending.append(
                    remote(side_of(me), side_of(me), side_send.at[layer, row],
                           side_recv.at[layer, me], mate(z, row))
                )

        mine = acts[layer].at[pl.ds(me * own, main)]
        for m in range(1, zs):
            pending.append(
                remote(mine, mine, z_send.at[layer, m], z_recv.at[layer, z],
                       index(paired(z, m, zs), y, x))
            )

        def spread(m):
            zz = paired(z, m, zs)
            owner = index(zz, y, x)
            if m:
                shard = acts[layer].at[pl.ds(owner * own, main)]
                arrived(shard, z_recv.at[layer, zz])
            slot = 0
            for first in (True, False):
                for n in range(1, ys):
                    part = 0 if first else 1
                    pending.append(
                        remote(piece(owner, part), piece(owner, part),
                               half_send.at[layer, m, slot], half_recv.at[layer, owner, part],
                               index(z, paired(y, n, ys), x))
                    )
                    slot += 1
                for n in range(1, xs):
                    part = 1 if first else 0
                    pending.append(
                        remote(piece(owner, part), piece(owner, part),
                               half_send.at[layer, m, slot], half_recv.at[layer, owner, part],
                               index(z, y, paired(x, n, xs)))
                    )
                    slot += 1

        def relay(m):
            zz = paired(z, m, zs)
            slot = 0
            for n in range(1, ys):
                owner = index(zz, paired(y, n, ys), x)
                arrived(piece(owner, 0), half_recv.at[layer, owner, 0])
                for k in range(1, xs):
                    pending.append(
                        remote(piece(owner, 0), piece(owner, 0),
                               pass_send.at[layer, m, slot], half_recv.at[layer, owner, 0],
                               index(z, y, paired(x, k, xs)))
                    )
                    slot += 1
            for n in range(1, xs):
                owner = index(zz, y, paired(x, n, xs))
                arrived(piece(owner, 1), half_recv.at[layer, owner, 1])
                for k in range(1, ys):
                    pending.append(
                        remote(piece(owner, 1), piece(owner, 1),
                               pass_send.at[layer, m, slot], half_recv.at[layer, owner, 1],
                               index(z, paired(y, k, ys), x))
                    )
                    slot += 1

        spread(0)
        if side:
            side_along_z(me, len(mates))
            for row in range(len(mates)):
                owner = mate(z, row)
                arrived(side_of(owner), side_recv.at[layer, owner])
                side_along_z(owner, row)
        if layer == 0:
            make_tables()
            place_in[me] = place[(me * own) // 128]
            to_table = pltpu.make_async_copy(table_out, table, smem_sem)
            to_table.start()
            to_table.wait()

            def send_place(t, carry):
                place_copy(t).start()
                return carry

            lax.fori_loop(0, devices - 1, send_place, 0)
        for m in range(1, zs):
            spread(m)
            relay(m - 1)
        relay(zs - 1)

        if side:
            for m in range(1, zs):
                zz = paired(z, m, zs)
                for owner in [index(zz, y, x)] + [mate(zz, row) for row in range(len(mates))]:
                    arrived(side_of(owner), side_recv.at[layer, owner])

        for m in range(zs):
            zz = paired(z, m, zs)
            for n in range(1, ys):
                owner = index(zz, paired(y, n, ys), x)
                arrived(piece(owner, 1), half_recv.at[layer, owner, 1])
            for n in range(1, xs):
                owner = index(zz, y, paired(x, n, xs))
                arrived(piece(owner, 0), half_recv.at[layer, owner, 0])
            for n in range(1, ys):
                for k in range(1, xs):
                    owner = index(zz, paired(y, n, ys), paired(x, k, xs))
                    for part in range(2):
                        arrived(piece(owner, part), half_recv.at[layer, owner, part])
        loads[layer].wait()

        def product(target, k, kind):
            at = target * capacity + k
            block = acts[layer][table[2 * layer, 0, at]]
            tile = weights[layer][table[2 * layer + 1, 0, at]]
            return jnp.dot(block, tile, preferred_element_type=jnp.float32).astype(kind)

        def buffers(is_far):
            if is_far:
                return far_out[layer], far_in[layer], 0
            return near_out[layer], near_in[layer], far

        def part_copy(t, is_far):
            sent, got, base = buffers(is_far)
            rows = pl.ds((t - base) * capacity, capacity)
            return pltpu.make_async_remote_copy(
                src_ref=sent.at[rows], dst_ref=got.at[rows],
                send_sem=part_send.at[layer, t], recv_sem=part_recv.at[layer, t],
                device_id={"neuron": partner(t)}, device_id_type=pl.DeviceIdType.MESH,
            )

        def fill(t, is_far, to):
            target = partner(t)
            base = buffers(is_far)[2]
            for k in range(capacity):
                to[(t - base) * capacity + k] = product(target, k, to.dtype)

        group = GROUP if far % GROUP == 0 else 1

        def step(is_far, base, g, carry):
            for i in range(group):
                fill(base + g * group + i, is_far, buffers(is_far)[0])
            for i in range(group):
                part_copy(base + g * group + i, is_far).start()
            return carry

        lax.fori_loop(0, far // group, functools.partial(step, True, 0), 0)
        lax.fori_loop(0, far // group - 1, functools.partial(step, False, far), 0)
        for t in range(devices - group, devices - 1):
            fill(t, False, near_out[layer])
        for t in range(devices - group, devices - 1):
            part_copy(t, False).start()
        fill(devices - 1, False, near_in[layer])

        if layer == 0:
            def take_place(t, carry):
                ref = place_in.at[partner(t)]
                pltpu.make_async_copy(ref, ref, place_recv.at[partner(t)]).wait()
                return carry

            lax.fori_loop(0, devices - 1, take_place, 0)
            to_smem = pltpu.make_async_copy(place_in, place_smem, smem_sem)
            to_smem.start()
            to_smem.wait()

        def take_part(is_far, t, carry):
            part_copy(t, is_far).wait_recv()
            return carry

        def terms(c, total, first):
            for t in range(first, first + far):
                at = place_smem[partner(t), layer, 0, chunk_at + c]
                total = total + buffers(t < far)[1][at].astype(jnp.float32)
            return total

        def combine_near(c, carry):
            start = jnp.broadcast_to(
                bias[pl.ds(layer, 1), pl.ds(pl.multiple_of(c * 128, 128), 128)],
                near_in[layer].shape[1:],
            )
            sums[c] = terms(c, start, far)
            return carry

        if layer == 0:
            early[1].wait()
        lax.fori_loop(far, devices - 1, functools.partial(take_part, False), 0)
        lax.fori_loop(0, own, combine_near, 0)
        lax.fori_loop(0, far, functools.partial(take_part, True), 0)

        def combine(c, carry):
            total = terms(c, sums[c], 0)
            value = jnp.minimum(jnp.maximum(total, 0.0), CEILING).astype(jnp.bfloat16)
            if layer + 1 < layers:
                acts[layer + 1][me * own + c] = value
            else:
                out[:, pl.ds(pl.multiple_of(c * 128, 128), 128)] = value
            return carry

        lax.fori_loop(0, own, combine, 0)

        for copy in pending:
            copy.wait_send()

        def drain(is_far, t, carry):
            part_copy(t, is_far).wait_send()
            if layer == 0:
                place_copy(t).wait_send()
            return carry

        lax.fori_loop(0, far, functools.partial(drain, True), 0)
        lax.fori_loop(far, devices - 1, functools.partial(drain, False), 0)


def local(images, tile_weights, tile_blocks, tile_count, bias):
    devices = lax.axis_size("neuron")
    layers, slot_total, block, _ = tile_weights.shape
    image_rows, local_width = images.shape
    own = local_width // block
    capacity = max(2, slot_total // devices)
    slots = devices * capacity
    zs, ys, xs = sides(devices)
    half_slots = slots // 2
    chunks = devices * own // 128
    fan = 2 * (ys + xs)
    vmem = pl.BlockSpec(memory_space=pltpu.VMEM)
    hbm = pl.BlockSpec(memory_space=pltpu.HBM)
    return pl.pallas_call(
        functools.partial(kernel, layers, devices, own, capacity),
        out_shape=jax.ShapeDtypeStruct((image_rows, local_width), jnp.bfloat16),
        in_specs=[
            pl.BlockSpec(memory_space=pltpu.SMEM), vmem, hbm, hbm, hbm,
        ],
        out_specs=vmem,
        scratch_shapes=[
            [pltpu.VMEM((devices * own, image_rows, block), jnp.bfloat16)] * layers,
            [pltpu.VMEM((slot_total, block, block), jnp.bfloat16)] * layers,
            [pltpu.VMEM((half_slots, image_rows, block), FAR)] * layers,
            [pltpu.VMEM((half_slots, image_rows, block), NEAR)] * layers,
            [pltpu.VMEM((half_slots + 1, image_rows, block), FAR)] * layers,
            [pltpu.VMEM((half_slots + 1, image_rows, block), NEAR)] * layers,
            pltpu.VMEM((2 * layers, 1, slots), jnp.int32),
            pltpu.SMEM((2 * layers, 1, slots), jnp.int32),
            pltpu.VMEM((chunks, layers, 1, 128), jnp.int32),
            pltpu.VMEM((devices, layers, 1, 128), jnp.int32),
            pltpu.SMEM((devices, layers, 1, 128), jnp.int32),
            pltpu.VMEM((image_rows, local_width), jnp.bfloat16),
            pltpu.VMEM((layers, local_width), jnp.float32),
            pltpu.VMEM((own, image_rows, block), jnp.float32),
            pltpu.SemaphoreType.DMA((2,)),
            pltpu.SemaphoreType.DMA((layers,)),
            pltpu.SemaphoreType.DMA((devices,)),
            pltpu.SemaphoreType.DMA((devices,)),
            pltpu.SemaphoreType.DMA,
            pltpu.SemaphoreType.DMA((layers, zs)),
            pltpu.SemaphoreType.DMA((layers, zs)),
            pltpu.SemaphoreType.DMA((layers, zs, fan)),
            pltpu.SemaphoreType.DMA((layers, devices, 2)),
            pltpu.SemaphoreType.DMA((layers, zs, 2 * ys * xs)),
            pltpu.SemaphoreType.DMA((layers, devices)),
            pltpu.SemaphoreType.DMA((layers, devices)),
            pltpu.SemaphoreType.DMA((layers, ys * xs)),
            pltpu.SemaphoreType.DMA((layers, ys * xs, zs)),
            pltpu.SemaphoreType.DMA((layers, devices)),
        ],
        compiler_params=pltpu.CompilerParams(
            collective_id=0, has_side_effects=True, vmem_limit_bytes=67043328
        ),
    )(tile_count.reshape(-1), jnp.transpose(tile_blocks, (0, 2, 1)), images, tile_weights, bias)


def solution(mesh):
    in_specs = (
        P("batch", "neuron"),
        P(None, "neuron", None, None),
        P(None, "neuron", None),
        P(None, "neuron"),
        P(None, "neuron"),
    )
    out_specs = P("batch", "neuron")
    return jax.shard_map(local, mesh=mesh, in_specs=in_specs, out_specs=out_specs, check_vma=False)
```
